32 devices in a mesh: rows: 4 (over y, x), cols: 2 (over core), slabs: 4 (over z).
Axes of the slice: x: 2, y: 2, z: 4, core: 2. Of those that a mesh axis runs over, the one named last changes fastest.
Arguments:
- field_values: float32 [16, 64, 512, 128], P('rows', 'cols', 'slabs'), may hold values from 0.5 to 2
- mobility: float32 [16, 64, 512, 128], P('rows', 'cols', 'slabs'), may hold values from 0.03 to 0.15
- source: float32 [16, 64, 512, 128], P('rows', 'cols', 'slabs'), may hold values from -0.2 to 0.2
Outputs:
- anomaly: float32 [16, 64, 512, 128], P('rows', 'cols', 'slabs')
- field_values_end: float32 [16, 64, 512, 128], P('rows', 'cols', 'slabs')
The draws below stay inside these ranges and needn't reach their ends.
All inputs are finite; a program needn't handle non-finite values.
Results may differ from the reference program's by a relative error of at most 0.00002.
Values sent between devices are 32-bit elements; how exact they have to be, the bound alone decides.
A program may use at most 128 MiB of HBM per device.

```python
import jax
import jax.numpy as jnp
from jax import lax

GRID_Y = 16
GRID_X = 64
GRID_Z = 512
LEVELS = 128
STEPS = 3


def shard_levels(stream_key, shape, split, least, largest):
    factor_of = 1.0
    for axis_at, shards_of in split:
        steps = jax.random.uniform(jax.random.fold_in(jax.random.fold_in(stream_key, 6), axis_at), (shards_of,), jnp.float32, least / len(split), largest / len(split))
        factor_of = factor_of * jnp.repeat(jnp.exp(steps), shape[axis_at] // shards_of).reshape((-1,) + (1,) * (len(shape) - 1 - axis_at))
    return factor_of


def setup_inputs(seed: int = 0) -> dict:
    splits = jax.random.split(jax.random.key(seed), 4)
    return {
        "field_values": jnp.clip(0.5 + 1.5 * jax.random.uniform(splits[0], (GRID_Y, GRID_X, GRID_Z, LEVELS), jnp.float32) ** shard_levels(splits[0], (GRID_Y, GRID_X, GRID_Z, LEVELS), ((0, 4), (1, 2), (2, 4)), -0.2, 0.2), 0.5, 2.0),
        "mobility": jnp.clip(0.03 + 0.120000007 * jax.random.uniform(splits[1], (GRID_Y, GRID_X, GRID_Z, LEVELS), jnp.float32) ** shard_levels(splits[1], (GRID_Y, GRID_X, GRID_Z, LEVELS), ((0, 4), (1, 2), (2, 4)), -0.2, 0.2), 0.03, 0.15),
        "source": jnp.clip(jax.random.uniform(splits[2], (GRID_Y, GRID_X, GRID_Z, LEVELS), jnp.float32, -0.2, 0.2) * shard_levels(splits[2], (GRID_Y, GRID_X, GRID_Z, LEVELS), ((0, 4), (1, 2), (2, 4)), -0.4, 0.0), -0.2, 0.2),
    }


def strip_edges(values, dims):
    for dim in dims:
        values = lax.slice_in_dim(values, 1, values.shape[dim] - 1, axis=dim)
    return values

def neighbour(values, dim, start, dims):
    others = [other for other in dims if other != dim]
    values = strip_edges(values, others)
    return lax.slice_in_dim(values, start, start + values.shape[dim] - 2, axis=dim)

def one_step(padded, mobility, source):
    middle = strip_edges(padded, (0, 1, 2))
    lower = [neighbour(padded, dim, 0, (0, 1, 2)) for dim in (0, 1, 2)]
    upper = [neighbour(padded, dim, 2, (0, 1, 2)) for dim in (0, 1, 2)]
    spread = lower[0] + upper[0] + lower[1] + upper[1] + lower[2] + upper[2] - 6.0 * middle
    return middle + mobility * spread + source

def reference(field_values, mobility, source):
    for step in range(STEPS):
        field_values = one_step(jnp.pad(field_values, ((1, 1), (1, 1), (1, 1), (0, 0)), mode='wrap'), mobility, source)
    line_mean = lax.optimization_barrier(jnp.mean(field_values, axis=2, keepdims=True))
    centred = field_values - line_mean
    line_variance = lax.optimization_barrier(jnp.mean(centred * centred, axis=2, keepdims=True))
    anomaly = centred * lax.rsqrt(line_variance + 0.0001)
    return (anomaly, field_values)
```

```python
import functools

import jax
import jax.numpy as jnp
from jax import lax
from jax.experimental import pallas as pl
from jax.experimental.pallas import tpu as pltpu
from jax.sharding import PartitionSpec as P

STEPS = 3
MESH = pl.DeviceIdType.MESH


def steps_kernel(
    sizes, spans, f, m, s, out, lines,
    field, mob, src, z_in, z_out, stats, stats_in, tail, tail_in,
    y_send, y_recv, w_send, w_recv, x_send, x_recv, z_send, z_recv, s_send, s_recv, e_send, e_recv, load_sem,
):
    planes, width, depth, _ = f.shape
    rows, cols, slabs = sizes
    chunks = len(spans)
    last = planes - 1
    short = spans[-1][1]

    def shifted(axis, by):
        count = lax.axis_size(axis)
        return {axis: lax.rem(lax.axis_index(axis) + by + count, count)}

    peers = [(axis, 1) for axis in ("rows", "cols")]
    peers += [(axis, -1) for axis, n in (("rows", rows), ("cols", cols)) if n > 2]
    peers += [("slabs", by) for by in range(1, slabs)]
    barrier = pltpu.get_barrier_semaphore()
    for axis, by in peers:
        pl.semaphore_signal(barrier, inc=1, device_id=shifted(axis, by), device_id_type=MESH)
    ends = (0, last)
    early = spans[0][1]

    def load(array, p, part=0):
        if array == 0:
            first, count = (0, early) if part == 0 else (early, width - early)
            return pltpu.make_async_copy(
                f.at[p, pl.ds(first, count)], field.at[0, p + 1, pl.ds(1 + first, count)],
                load_sem.at[3 * part, p])
        if array == 1:
            return pltpu.make_async_copy(m.at[p], mob.at[p], load_sem.at[1, p])
        return pltpu.make_async_copy(s.at[p], src.at[p], load_sem.at[2, p])

    inner = tuple(range(1, last))
    for part in (0, 1):
        for p in ends:
            load(0, p, part).start()
    for p in inner:
        for part in (0, 1):
            load(0, p, part).start()
    for array in (1, 2):
        for p in range(planes):
            load(array, p).start()
    pl.semaphore_wait(barrier, len(peers))

    def remote(source, target, send, recv, device):
        return pltpu.make_async_remote_copy(
            src_ref=source, dst_ref=target, send_sem=send, recv_sem=recv,
            device_id=device, device_id_type=MESH,
        )

    def y_copy(t, side, k, less=0):
        plane = last * (1 - side)
        first, count = spans[k]
        count -= less
        span = pl.ds(1 + first, count)
        source = field.at[t % 2, plane + 1, span]
        target = field.at[t % 2, (planes + 1) * side, span]
        return remote(source, target, y_send.at[t, side, k], y_recv.at[t, side, k],
                      shifted("rows", 1 - 2 * side))

    def x_copy(t, side, p):
        x = width - 1 if side == 0 else 0
        source = field.at[t % 2, p + 1, x + 1]
        target = field.at[t % 2, p + 1, 0 if side == 0 else width + 1]
        return remote(source, target, x_send.at[t, side, p], x_recv.at[t, side, p],
                      shifted("cols", 1 if side == 0 else -1))

    def z_copy(t, side, p):
        return remote(z_out.at[t, side, p], z_in.at[t, side, p],
                      z_send.at[t, side, p], z_recv.at[t, side, p],
                      shifted("slabs", 1 if side == 0 else -1))

    def s_copy(by, p):
        return remote(stats.at[p], stats_in.at[by - 1, p],
                      s_send.at[by - 1, p], s_recv.at[by - 1, p], shifted("slabs", by))

    def e_copy(by):
        return remote(tail, tail_in.at[by - 1], e_send.at[by - 1], e_recv.at[by - 1],
                      shifted("slabs", by))

    odd = lax.rem(lax.axis_index("rows"), 2)
    sides = [lax.rem(odd + i, 2) for i in range(2)]
    second = lax.rem(lax.axis_index("cols"), 2) == 1
    forward = cols % 2 == 0 and spans[-1][1] > 1

    def w_copy(side):
        plane = last * (1 - side)
        return remote(field.at[0, plane + 1, 0], field.at[0, (planes + 1) * side, width],
                      w_send.at[side], w_recv.at[side],
                      {"rows": shifted("rows", 1 - 2 * side)["rows"],
                       "cols": shifted("cols", -1)["cols"]})

    def on_last(act):
        if not forward:
            act(0, False)
            return
        pl.when(second)(lambda: act(0, False))
        pl.when(jnp.logical_not(second))(lambda: act(1, True))

    for part in (0, 1):
        for p in ends:
            load(0, p, part).wait()
        for k in ((0,), range(1, chunks - 1))[part]:
            for side in sides:
                y_copy(0, 1 - side, k).start()
    for p in ends + inner:
        if p in inner:
            for part in (0, 1):
                load(0, p, part).wait()
        for side in (0, 1):
            x_copy(0, side, p).start()

    for p in ends:
        x_copy(0, 0, p).wait_recv()

    def send_last(less, _):
        for side in sides:
            y_copy(0, 1 - side, chunks - 1, less).start()

    if forward:
        @pl.when(second)
        def _():
            for side in sides:
                w_copy(1 - side).start()
    on_last(send_last)

    for p in range(planes):

        def edge(x, _):
            z_out[0, 0, p, pl.ds(x, 1)] = field[0, p + 1, x + 1, depth - 1:depth]
            z_out[0, 1, p, pl.ds(x, 1)] = field[0, p + 1, x + 1, 0:1]
            return 0

        lax.fori_loop(0, width, edge, 0)
        for side in (0, 1):
            z_copy(0, side, p).start()
    for array in (1, 2):
        for p in range(planes):
            load(array, p).wait()

    def compute(t, p, first, count, at=None):
        now, after = t % 2, (t + 1) % 2

        def row(x, _):
            c = field[now, p + 1, x + 1]
            level = lax.broadcasted_iota(jnp.int32, c.shape, 0)
            low = jnp.where(level == 0, z_in[t, 0, p, pl.ds(x, 1)], pltpu.roll(c, 1, 0))
            high = jnp.where(level == depth - 1, z_in[t, 1, p, pl.ds(x, 1)],
                             pltpu.roll(c, depth - 1, 0))
            spread = (field[now, p, x + 1] + field[now, p + 2, x + 1]
                      + field[now, p + 1, x] + field[now, p + 1, x + 2] + low + high - 6.0 * c)
            new = c + mob[p, x] * spread + src[p, x]
            if t + 1 < STEPS:
                field[after, p + 1, x + 1] = new
                z_out[t + 1, 0, p, pl.ds(x, 1)] = new[depth - 1:depth]
                z_out[t + 1, 1, p, pl.ds(x, 1)] = new[0:1]
            else:
                out[p, x] = new
                mean = jnp.sum(new, axis=0, keepdims=True) * (1.0 / depth)
                moved = new - mean
                squares = jnp.sum(moved * moved, axis=0, keepdims=True)
                if at is not None:
                    tail[at, 0, pl.ds(x - first, 1)] = mean
                    tail[at, 1, pl.ds(x - first, 1)] = squares
                else:
                    stats[p, 0, pl.ds(x, 1)] = mean
                    stats[p, 1, pl.ds(x, 1)] = squares
            return 0

        lax.fori_loop(first, first + count, row, 0)

    def ready(t, p):
        for side in (0, 1):
            if t or side or p not in ends:
                x_copy(t, side, p).wait_recv()
            z_copy(t, side, p).wait_recv()
            if t >= 1:
                x_copy(t - 1, side, p).wait_send()

    def finish(t, p):
        if t + 1 < STEPS:
            for side in (0, 1):
                x_copy(t + 1, side, p).start()
                z_copy(t + 1, side, p).start()
        else:
            for by in range(1, slabs):
                s_copy(by, p).start()

    def combined(own, others):
        total = own[0]
        for other in others:
            total = total + other[0]
        mean = total * (1.0 / slabs)
        away = own[0] - mean
        squares, between = own[1], away * away
        for other in others:
            away = other[0] - mean
            squares, between = squares + other[1], between + away * away
        variance = (squares + depth * between) * (1.0 / (depth * slabs))
        return mean, lax.rsqrt(variance + 0.0001)

    def settle(p):
        for by in range(1, slabs):
            s_copy(by, p).wait_recv()
        lines[p, 0], lines[p, 1] = combined(
            (stats[p, 0], stats[p, 1]),
            [(stats_in[i, p, 0], stats_in[i, p, 1]) for i in range(slabs - 1)])

    for p in (0, last):
        stats[p] = jnp.zeros_like(stats[p])
    for t in range(STEPS):
        for p in range(1, last):
            ready(t, p)
            compute(t, p, 0, width)
            finish(t, p)
        ready(t, 0)
        ready(t, last)
        for k in range(chunks):
            tailed = t + 1 == STEPS and k + 1 == chunks
            if tailed:
                finish(t, 0)
                finish(t, last)
                for p in range(1, last):
                    settle(p)
            for side in sides:
                p = side * last
                if t == 0 and k + 1 == chunks:

                    def arrive(less, passed, side=side):
                        y_copy(0, side, chunks - 1, less).wait_recv()
                        if passed:
                            w_copy(side).wait_recv()

                    on_last(arrive)
                else:
                    y_copy(t, side, k).wait_recv()
                if t == 1 and k + 1 == chunks:

                    def left(less, _, side=side):
                        y_copy(0, 1 - side, chunks - 1, less).wait_send()

                    on_last(left)
                elif t >= 1:
                    y_copy(t - 1, 1 - side, k).wait_send()
                compute(t, p, spans[k][0], spans[k][1], side if tailed else None)
                if t + 1 < STEPS:
                    y_copy(t + 1, 1 - side, k).start()
        if t == 0 and forward:

            @pl.when(second)
            def _():
                for side in (0, 1):
                    w_copy(side).wait_send()

        if t + 1 < STEPS:
            finish(t, 0)
            finish(t, last)

    for by in range(1, slabs):
        e_copy(by).start()
    settle(0)
    settle(last)
    for by in range(1, slabs):
        e_copy(by).wait_recv()
    for side, p in ((0, 0), (1, last)):
        mean, scale = combined(
            (tail[side, 0], tail[side, 1]),
            [(tail_in[i, side, 0], tail_in[i, side, 1]) for i in range(slabs - 1)])
        lines[p, 0, width - short:width] = mean
        lines[p, 1, width - short:width] = scale

    for side in (0, 1):
        for k in range(chunks):
            y_copy(STEPS - 1, side, k).wait_send()
        for p in range(planes):
            x_copy(STEPS - 1, side, p).wait_send()
            for t in range(STEPS):
                z_copy(t, side, p).wait_send()
    for p in range(planes):
        for by in range(1, slabs):
            s_copy(by, p).wait_send()
    for by in range(1, slabs):
        e_copy(by).wait_send()


def scale_kernel(
    part, block, line, anomaly, out, scaled, out_sem, anomaly_sem
):
    planes, width = block.shape[:2]
    pieces = [(p, first) for p in range(planes) for first in range(0, width, part)]

    def copy(source, target, sems, i):
        p, first = pieces[i]
        at = (p, pl.ds(first, part))
        return pltpu.make_async_copy(source.at[at], target.at[at], sems.at[i])

    for i in range(len(pieces)):
        copy(block, out, out_sem, i).start()
    for i, (p, first) in enumerate(pieces):

        def row(x, _):
            centred = block[p, x] - line[p, 0, pl.ds(x, 1)]
            scaled[p, x] = centred * line[p, 1, pl.ds(x, 1)]
            return 0

        lax.fori_loop(first, first + part, row, 0)
        copy(scaled, anomaly, anomaly_sem, i).start()
    for i in range(len(pieces)):
        copy(block, out, out_sem, i).wait()
        copy(scaled, anomaly, anomaly_sem, i).wait()


def spans_of(width):
    size, first, spans = max(width // 4, 1), 0, []
    while first < width:
        if width - first <= size:
            size = max((width - first) // 2, min(2, width - first))
        spans.append((first, size))
        first += size
    return tuple(spans)


def per_device(sizes, field_values, mobility, source):
    planes, width, depth, levels = field_values.shape
    slabs = sizes[2]
    spans = spans_of(width)
    chunks, short = len(spans), spans[-1][1]
    f32 = jnp.float32
    dma = pltpu.SemaphoreType.DMA
    any_space = pl.BlockSpec(memory_space=pl.ANY)
    held = pl.BlockSpec(memory_space=pltpu.VMEM)
    line = (planes, 2, width, levels)
    whole = jax.ShapeDtypeStruct(field_values.shape, f32)
    end, lines = pl.pallas_call(
        functools.partial(steps_kernel, sizes, spans),
        out_shape=(pltpu.VMEM(field_values.shape, f32), pltpu.VMEM(line, f32)),
        in_specs=[any_space] * 3,
        out_specs=(held, held),
        scratch_shapes=[
            pltpu.VMEM((2, planes + 2, width + 2, depth, levels), f32),
            pltpu.VMEM(field_values.shape, f32),
            pltpu.VMEM(field_values.shape, f32),
            pltpu.VMEM((STEPS, 2, planes, width, levels), f32),
            pltpu.VMEM((STEPS, 2, planes, width, levels), f32),
            pltpu.VMEM(line, f32),
            pltpu.VMEM((slabs - 1,) + line, f32),
            pltpu.VMEM((2, 2, short, levels), f32),
            pltpu.VMEM((slabs - 1, 2, 2, short, levels), f32),
            dma((STEPS, 2, chunks)), dma((STEPS, 2, chunks)),
            dma((2,)), dma((2,)),
            dma((STEPS, 2, planes)), dma((STEPS, 2, planes)),
            dma((STEPS, 2, planes)), dma((STEPS, 2, planes)),
            dma((slabs - 1, planes)), dma((slabs - 1, planes)),
            dma((slabs - 1,)), dma((slabs - 1,)),
            dma((4, planes)),
        ],
        compiler_params=pltpu.CompilerParams(
            collective_id=0, has_side_effects=True, vmem_limit_bytes=46 * 1024 * 1024),
    )(field_values, mobility, source)

    part = max(width // 4, 1)
    pieces = planes * (width // part)
    return pl.pallas_call(
        functools.partial(scale_kernel, part),
        out_shape=(whole, whole),
        in_specs=[held, held],
        out_specs=(any_space, any_space),
        scratch_shapes=[
            pltpu.VMEM(field_values.shape, f32),
            dma((pieces,)), dma((pieces,)),
        ],
        compiler_params=pltpu.CompilerParams(vmem_limit_bytes=20 * 1024 * 1024),
    )(end, lines)


def solution(mesh):
    sizes = tuple(mesh.shape[axis] for axis in ("rows", "cols", "slabs"))
    spec = P("rows", "cols", "slabs", None)
    return jax.shard_map(
        functools.partial(per_device, sizes),
        mesh=mesh,
        in_specs=(spec, spec, spec),
        out_specs=(spec, spec),
        check_vma=False,
    )
```

```python
import functools

import jax
import jax.numpy as jnp
from jax import lax
from jax.experimental import pallas as pl
from jax.experimental.pallas import tpu as pltpu
from jax.sharding import PartitionSpec as P

STEPS = 3
MESH = pl.DeviceIdType.MESH


def steps_kernel(
    sizes, spans, f, m, s, out, lines,
    field, mob, src, z_in, z_out, stats, stats_in, tail, tail_in,
    y_send, y_recv, w_send, w_recv, x_send, x_recv, z_send, z_recv, s_send, s_recv, e_send, e_recv, load_sem,
):
    planes, width, depth, _ = f.shape
    rows, cols, slabs = sizes
    chunks = len(spans)
    last = planes - 1
    short = spans[-1][1]

    def shifted(axis, by):
        count = lax.axis_size(axis)
        return {axis: lax.rem(lax.axis_index(axis) + by + count, count)}

    peers = [(axis, 1) for axis in ("rows", "cols")]
    peers += [(axis, -1) for axis, n in (("rows", rows), ("cols", cols)) if n > 2]
    peers += [("slabs", by) for by in range(1, slabs)]
    barrier = pltpu.get_barrier_semaphore()
    for axis, by in peers:
        pl.semaphore_signal(barrier, inc=1, device_id=shifted(axis, by), device_id_type=MESH)
    ends = (0, last)
    early = spans[0][1]

    def load(array, p, part=0):
        if array == 0:
            first, count = (0, early) if part == 0 else (early, width - early)
            return pltpu.make_async_copy(
                f.at[p, pl.ds(first, count)], field.at[0, p + 1, pl.ds(1 + first, count)],
                load_sem.at[3 * part, p])
        if array == 1:
            return pltpu.make_async_copy(m.at[p], mob.at[p], load_sem.at[1, p])
        return pltpu.make_async_copy(s.at[p], src.at[p], load_sem.at[2, p])

    inner = tuple(range(1, last))
    for part in (0, 1):
        for p in ends:
            load(0, p, part).start()
    for p in inner:
        for part in (0, 1):
            load(0, p, part).start()
    for array in (1, 2):
        for p in range(planes):
            load(array, p).start()
    pl.semaphore_wait(barrier, len(peers))

    def remote(source, target, send, recv, device):
        return pltpu.make_async_remote_copy(
            src_ref=source, dst_ref=target, send_sem=send, recv_sem=recv,
            device_id=device, device_id_type=MESH,
        )

    def y_copy(t, side, k, less=0):
        plane = last * (1 - side)
        first, count = spans[k]
        count -= less
        span = pl.ds(1 + first, count)
        source = field.at[t % 2, plane + 1, span]
        target = field.at[t % 2, (planes + 1) * side, span]
        return remote(source, target, y_send.at[t, side, k], y_recv.at[t, side, k],
                      shifted("rows", 1 - 2 * side))

    def x_copy(t, side, p):
        x = width - 1 if side == 0 else 0
        source = field.at[t % 2, p + 1, x + 1]
        target = field.at[t % 2, p + 1, 0 if side == 0 else width + 1]
        return remote(source, target, x_send.at[t, side, p], x_recv.at[t, side, p],
                      shifted("cols", 1 if side == 0 else -1))

    def z_copy(t, side, p):
        return remote(z_out.at[t, side, p], z_in.at[t, side, p],
                      z_send.at[t, side, p], z_recv.at[t, side, p],
                      shifted("slabs", 1 if side == 0 else -1))

    def s_copy(by, p):
        return remote(stats.at[p], stats_in.at[by - 1, p],
                      s_send.at[by - 1, p], s_recv.at[by - 1, p], shifted("slabs", by))

    def e_copy(by):
        return remote(tail, tail_in.at[by - 1], e_send.at[by - 1], e_recv.at[by - 1],
                      shifted("slabs", by))

    wraps = (lax.rem(lax.axis_index("rows") + 1, rows) < 2).astype(jnp.int32)
    sides = [lax.rem(wraps + i, 2) for i in range(2)]
    second = lax.rem(lax.axis_index("cols"), 2) == 1
    forward = cols % 2 == 0 and spans[-1][1] > 1

    def w_copy(side):
        plane = last * (1 - side)
        return remote(field.at[0, plane + 1, 0], field.at[0, (planes + 1) * side, width],
                      w_send.at[side], w_recv.at[side],
                      {"rows": shifted("rows", 1 - 2 * side)["rows"],
                       "cols": shifted("cols", -1)["cols"]})

    def on_last(act):
        if not forward:
            act(0, False)
            return
        pl.when(second)(lambda: act(0, False))
        pl.when(jnp.logical_not(second))(lambda: act(1, True))

    for part in (0, 1):
        for p in ends:
            load(0, p, part).wait()
        for k in ((0,), range(1, chunks - 1))[part]:
            for side in sides:
                y_copy(0, 1 - side, k).start()
    for p in ends + inner:
        if p in inner:
            for part in (0, 1):
                load(0, p, part).wait()
        for side in (0, 1):
            x_copy(0, side, p).start()

    for p in ends:
        x_copy(0, 0, p).wait_recv()

    def send_last(less, _):
        for side in sides:
            y_copy(0, 1 - side, chunks - 1, less).start()

    if forward:
        @pl.when(second)
        def _():
            for side in sides:
                w_copy(1 - side).start()
    on_last(send_last)

    for p in range(planes):

        def edge(x, _):
            z_out[0, 0, p, pl.ds(x, 1)] = field[0, p + 1, x + 1, depth - 1:depth]
            z_out[0, 1, p, pl.ds(x, 1)] = field[0, p + 1, x + 1, 0:1]
            return 0

        lax.fori_loop(0, width, edge, 0)
        for side in (0, 1):
            z_copy(0, side, p).start()
    for array in (1, 2):
        for p in range(planes):
            load(array, p).wait()

    def compute(t, p, first, count, at=None):
        now, after = t % 2, (t + 1) % 2

        def row(x, _):
            c = field[now, p + 1, x + 1]
            level = lax.broadcasted_iota(jnp.int32, c.shape, 0)
            low = jnp.where(level == 0, z_in[t, 0, p, pl.ds(x, 1)], pltpu.roll(c, 1, 0))
            high = jnp.where(level == depth - 1, z_in[t, 1, p, pl.ds(x, 1)],
                             pltpu.roll(c, depth - 1, 0))
            spread = (field[now, p, x + 1] + field[now, p + 2, x + 1]
                      + field[now, p + 1, x] + field[now, p + 1, x + 2] + low + high - 6.0 * c)
            new = c + mob[p, x] * spread + src[p, x]
            if t + 1 < STEPS:
                field[after, p + 1, x + 1] = new
                z_out[t + 1, 0, p, pl.ds(x, 1)] = new[depth - 1:depth]
                z_out[t + 1, 1, p, pl.ds(x, 1)] = new[0:1]
            else:
                out[p, x] = new
                mean = jnp.sum(new, axis=0, keepdims=True) * (1.0 / depth)
                moved = new - mean
                squares = jnp.sum(moved * moved, axis=0, keepdims=True)
                if at is not None:
                    tail[at, 0, pl.ds(x - first, 1)] = mean
                    tail[at, 1, pl.ds(x - first, 1)] = squares
                else:
                    stats[p, 0, pl.ds(x, 1)] = mean
                    stats[p, 1, pl.ds(x, 1)] = squares
            return 0

        lax.fori_loop(first, first + count, row, 0)

    def ready(t, p):
        for side in (0, 1):
            if t or side or p not in ends:
                x_copy(t, side, p).wait_recv()
            z_copy(t, side, p).wait_recv()
            if t >= 1:
                x_copy(t - 1, side, p).wait_send()

    def finish(t, p):
        if t + 1 < STEPS:
            for side in (0, 1):
                x_copy(t + 1, side, p).start()
                z_copy(t + 1, side, p).start()
        else:
            for by in range(1, slabs):
                s_copy(by, p).start()

    def combined(own, others):
        total = own[0]
        for other in others:
            total = total + other[0]
        mean = total * (1.0 / slabs)
        away = own[0] - mean
        squares, between = own[1], away * away
        for other in others:
            away = other[0] - mean
            squares, between = squares + other[1], between + away * away
        variance = (squares + depth * between) * (1.0 / (depth * slabs))
        return mean, lax.rsqrt(variance + 0.0001)

    def settle(p):
        for by in range(1, slabs):
            s_copy(by, p).wait_recv()
        lines[p, 0], lines[p, 1] = combined(
            (stats[p, 0], stats[p, 1]),
            [(stats_in[i, p, 0], stats_in[i, p, 1]) for i in range(slabs - 1)])

    for p in (0, last):
        stats[p] = jnp.zeros_like(stats[p])
    for t in range(STEPS):
        for p in range(1, last):
            ready(t, p)
            compute(t, p, 0, width)
            finish(t, p)
        ready(t, 0)
        ready(t, last)
        for k in range(chunks):
            tailed = t + 1 == STEPS and k + 1 == chunks
            if tailed:
                finish(t, 0)
                finish(t, last)
                for p in range(1, last):
                    settle(p)
            for side in sides:
                p = side * last
                if t == 0 and k + 1 == chunks:

                    def arrive(less, passed, side=side):
                        y_copy(0, side, chunks - 1, less).wait_recv()
                        if passed:
                            w_copy(side).wait_recv()

                    on_last(arrive)
                else:
                    y_copy(t, side, k).wait_recv()
                if t == 1 and k + 1 == chunks:

                    def left(less, _, side=side):
                        y_copy(0, 1 - side, chunks - 1, less).wait_send()

                    on_last(left)
                elif t >= 1:
                    y_copy(t - 1, 1 - side, k).wait_send()
                compute(t, p, spans[k][0], spans[k][1], side if tailed else None)
                if t + 1 < STEPS:
                    y_copy(t + 1, 1 - side, k).start()
        if t == 0 and forward:

            @pl.when(second)
            def _():
                for side in (0, 1):
                    w_copy(side).wait_send()

        if t + 1 < STEPS:
            finish(t, 0)
            finish(t, last)

    for by in range(1, slabs):
        e_copy(by).start()
    settle(0)
    settle(last)
    for by in range(1, slabs):
        e_copy(by).wait_recv()
    for side, p in ((0, 0), (1, last)):
        mean, scale = combined(
            (tail[side, 0], tail[side, 1]),
            [(tail_in[i, side, 0], tail_in[i, side, 1]) for i in range(slabs - 1)])
        lines[p, 0, width - short:width] = mean
        lines[p, 1, width - short:width] = scale

    for side in (0, 1):
        for k in range(chunks):
            y_copy(STEPS - 1, side, k).wait_send()
        for p in range(planes):
            x_copy(STEPS - 1, side, p).wait_send()
            for t in range(STEPS):
                z_copy(t, side, p).wait_send()
    for p in range(planes):
        for by in range(1, slabs):
            s_copy(by, p).wait_send()
    for by in range(1, slabs):
        e_copy(by).wait_send()


def scale_kernel(
    part, block, line, anomaly, out, scaled, out_sem, anomaly_sem
):
    planes, width = block.shape[:2]
    pieces = [(p, first) for p in range(planes) for first in range(0, width, part)]

    def copy(source, target, sems, i):
        p, first = pieces[i]
        at = (p, pl.ds(first, part))
        return pltpu.make_async_copy(source.at[at], target.at[at], sems.at[i])

    for i in range(len(pieces)):
        copy(block, out, out_sem, i).start()
    for i, (p, first) in enumerate(pieces):

        def row(x, _):
            centred = block[p, x] - line[p, 0, pl.ds(x, 1)]
            scaled[p, x] = centred * line[p, 1, pl.ds(x, 1)]
            return 0

        lax.fori_loop(first, first + part, row, 0)
        copy(scaled, anomaly, anomaly_sem, i).start()
    for i in range(len(pieces)):
        copy(block, out, out_sem, i).wait()
        copy(scaled, anomaly, anomaly_sem, i).wait()


def spans_of(width):
    size, first, spans = max(width // 4, 1), 0, []
    while first < width:
        if width - first <= size:
            size = max((width - first) // 2, min(2, width - first))
        spans.append((first, size))
        first += size
    return tuple(spans)


def per_device(sizes, field_values, mobility, source):
    planes, width, depth, levels = field_values.shape
    slabs = sizes[2]
    spans = spans_of(width)
    chunks, short = len(spans), spans[-1][1]
    f32 = jnp.float32
    dma = pltpu.SemaphoreType.DMA
    any_space = pl.BlockSpec(memory_space=pl.ANY)
    held = pl.BlockSpec(memory_space=pltpu.VMEM)
    line = (planes, 2, width, levels)
    whole = jax.ShapeDtypeStruct(field_values.shape, f32)
    end, lines = pl.pallas_call(
        functools.partial(steps_kernel, sizes, spans),
        out_shape=(pltpu.VMEM(field_values.shape, f32), pltpu.VMEM(line, f32)),
        in_specs=[any_space] * 3,
        out_specs=(held, held),
        scratch_shapes=[
            pltpu.VMEM((2, planes + 2, width + 2, depth, levels), f32),
            pltpu.VMEM(field_values.shape, f32),
            pltpu.VMEM(field_values.shape, f32),
            pltpu.VMEM((STEPS, 2, planes, width, levels), f32),
            pltpu.VMEM((STEPS, 2, planes, width, levels), f32),
            pltpu.VMEM(line, f32),
            pltpu.VMEM((slabs - 1,) + line, f32),
            pltpu.VMEM((2, 2, short, levels), f32),
            pltpu.VMEM((slabs - 1, 2, 2, short, levels), f32),
            dma((STEPS, 2, chunks)), dma((STEPS, 2, chunks)),
            dma((2,)), dma((2,)),
            dma((STEPS, 2, planes)), dma((STEPS, 2, planes)),
            dma((STEPS, 2, planes)), dma((STEPS, 2, planes)),
            dma((slabs - 1, planes)), dma((slabs - 1, planes)),
            dma((slabs - 1,)), dma((slabs - 1,)),
            dma((4, planes)),
        ],
        compiler_params=pltpu.CompilerParams(
            collective_id=0, has_side_effects=True, vmem_limit_bytes=46 * 1024 * 1024),
    )(field_values, mobility, source)

    part = max(width // 4, 1)
    pieces = planes * (width // part)
    return pl.pallas_call(
        functools.partial(scale_kernel, part),
        out_shape=(whole, whole),
        in_specs=[held, held],
        out_specs=(any_space, any_space),
        scratch_shapes=[
            pltpu.VMEM(field_values.shape, f32),
            dma((pieces,)), dma((pieces,)),
        ],
        compiler_params=pltpu.CompilerParams(vmem_limit_bytes=20 * 1024 * 1024),
    )(end, lines)


def solution(mesh):
    sizes = tuple(mesh.shape[axis] for axis in ("rows", "cols", "slabs"))
    spec = P("rows", "cols", "slabs", None)
    return jax.shard_map(
        functools.partial(per_device, sizes),
        mesh=mesh,
        in_specs=(spec, spec, spec),
        out_specs=(spec, spec),
        check_vma=False,
    )
```

```python
import functools

import jax
import jax.numpy as jnp
from jax import lax
from jax.experimental import pallas as pl
from jax.experimental.pallas import tpu as pltpu
from jax.sharding import PartitionSpec as P

STEPS = 3
MESH = pl.DeviceIdType.MESH


def steps_kernel(
    sizes, spans, f, m, s, out, lines,
    field, mob, src, z_in, z_out, stats, stats_in, tail, tail_in,
    y_send, y_recv, w_send, w_recv, x_send, x_recv, z_send, z_recv, s_send, s_recv, e_send, e_recv, load_sem,
):
    planes, width, depth, _ = f.shape
    rows, cols, slabs = sizes
    chunks = len(spans)
    last = planes - 1
    short = spans[-1][1]

    def shifted(axis, by):
        count = lax.axis_size(axis)
        return {axis: lax.rem(lax.axis_index(axis) + by + count, count)}

    peers = [(axis, 1) for axis in ("rows", "cols")]
    peers += [(axis, -1) for axis, n in (("rows", rows), ("cols", cols)) if n > 2]
    peers += [("slabs", by) for by in range(1, slabs)]
    barrier = pltpu.get_barrier_semaphore()
    for axis, by in peers:
        pl.semaphore_signal(barrier, inc=1, device_id=shifted(axis, by), device_id_type=MESH)
    ends = (0, last)
    early = spans[0][1]

    def load(array, p, part=0):
        if array == 0:
            first, count = (0, early) if part == 0 else (early, width - early)
            return pltpu.make_async_copy(
                f.at[p, pl.ds(first, count)], field.at[0, p + 1, pl.ds(1 + first, count)],
                load_sem.at[3 * part, p])
        if array == 1:
            return pltpu.make_async_copy(m.at[p], mob.at[p], load_sem.at[1, p])
        return pltpu.make_async_copy(s.at[p], src.at[p], load_sem.at[2, p])

    inner = tuple(range(1, last))
    for p in ends:
        load(0, p).start()
    pl.semaphore_wait(barrier, len(peers))

    def remote(source, target, send, recv, device):
        return pltpu.make_async_remote_copy(
            src_ref=source, dst_ref=target, send_sem=send, recv_sem=recv,
            device_id=device, device_id_type=MESH,
        )

    def y_copy(t, side, k, less=0):
        plane = last * (1 - side)
        first, count = spans[k]
        count -= less
        span = pl.ds(1 + first, count)
        source = field.at[t % 2, plane + 1, span]
        target = field.at[t % 2, (planes + 1) * side, span]
        return remote(source, target, y_send.at[t, side, k], y_recv.at[t, side, k],
                      shifted("rows", 1 - 2 * side))

    def x_copy(t, side, p):
        x = width - 1 if side == 0 else 0
        source = field.at[t % 2, p + 1, x + 1]
        target = field.at[t % 2, p + 1, 0 if side == 0 else width + 1]
        return remote(source, target, x_send.at[t, side, p], x_recv.at[t, side, p],
                      shifted("cols", 1 if side == 0 else -1))

    def z_copy(t, side, p):
        return remote(z_out.at[t, side, p], z_in.at[t, side, p],
                      z_send.at[t, side, p], z_recv.at[t, side, p],
                      shifted("slabs", 1 if side == 0 else -1))

    def s_copy(by, p):
        return remote(stats.at[p], stats_in.at[by - 1, p],
                      s_send.at[by - 1, p], s_recv.at[by - 1, p], shifted("slabs", by))

    def e_copy(by):
        return remote(tail, tail_in.at[by - 1], e_send.at[by - 1], e_recv.at[by - 1],
                      shifted("slabs", by))

    wraps = (lax.rem(lax.axis_index("rows") + 1, rows) < 2).astype(jnp.int32)
    sides = [lax.rem(wraps + i, 2) for i in range(2)]
    second = lax.rem(lax.axis_index("cols"), 2) == 1
    forward = cols % 2 == 0 and spans[-1][1] > 1

    def w_copy(side):
        plane = last * (1 - side)
        return remote(field.at[0, plane + 1, 0], field.at[0, (planes + 1) * side, width],
                      w_send.at[side], w_recv.at[side],
                      {"rows": shifted("rows", 1 - 2 * side)["rows"],
                       "cols": shifted("cols", -1)["cols"]})

    def on_last(act):
        if not forward:
            act(0, False)
            return
        pl.when(second)(lambda: act(0, False))
        pl.when(jnp.logical_not(second))(lambda: act(1, True))

    for part in (0, 1):
        for p in ends:
            load(0, p, part).wait()
        for k in ((0,), range(1, chunks - 1))[part]:
            for side in sides:
                y_copy(0, 1 - side, k).start()
        if part == 0:
            for p in ends:
                load(0, p, 1).start()
            for p in inner:
                for late in (0, 1):
                    load(0, p, late).start()
    for p in ends + inner:
        if p in inner:
            for part in (0, 1):
                load(0, p, part).wait()
        for side in (0, 1):
            x_copy(0, side, p).start()

    for p in ends:
        x_copy(0, 0, p).wait_recv()

    def send_last(less, _):
        for side in sides:
            y_copy(0, 1 - side, chunks - 1, less).start()

    if forward:
        @pl.when(second)
        def _():
            for side in sides:
                w_copy(1 - side).start()
    on_last(send_last)

    for p in range(planes):

        def edge(x, _):
            z_out[0, 0, p, pl.ds(x, 1)] = field[0, p + 1, x + 1, depth - 1:depth]
            z_out[0, 1, p, pl.ds(x, 1)] = field[0, p + 1, x + 1, 0:1]
            return 0

        lax.fori_loop(0, width, edge, 0)
        for side in (0, 1):
            z_copy(0, side, p).start()
    for p in inner + ends:
        for array in (1, 2):
            load(array, p).start()
            load(array, p).wait()

    def compute(t, p, first, count, at=None):
        now, after = t % 2, (t + 1) % 2

        def row(x, _):
            c = field[now, p + 1, x + 1]
            level = lax.broadcasted_iota(jnp.int32, c.shape, 0)
            low = jnp.where(level == 0, z_in[t, 0, p, pl.ds(x, 1)], pltpu.roll(c, 1, 0))
            high = jnp.where(level == depth - 1, z_in[t, 1, p, pl.ds(x, 1)],
                             pltpu.roll(c, depth - 1, 0))
            spread = (field[now, p, x + 1] + field[now, p + 2, x + 1]
                      + field[now, p + 1, x] + field[now, p + 1, x + 2] + low + high - 6.0 * c)
            new = c + mob[p, x] * spread + src[p, x]
            if t + 1 < STEPS:
                field[after, p + 1, x + 1] = new
                z_out[t + 1, 0, p, pl.ds(x, 1)] = new[depth - 1:depth]
                z_out[t + 1, 1, p, pl.ds(x, 1)] = new[0:1]
            else:
                out[p, x] = new
                mean = jnp.sum(new, axis=0, keepdims=True) * (1.0 / depth)
                moved = new - mean
                squares = jnp.sum(moved * moved, axis=0, keepdims=True)
                if at is not None:
                    tail[at, 0, pl.ds(x - first, 1)] = mean
                    tail[at, 1, pl.ds(x - first, 1)] = squares
                else:
                    stats[p, 0, pl.ds(x, 1)] = mean
                    stats[p, 1, pl.ds(x, 1)] = squares
            return 0

        lax.fori_loop(first, first + count, row, 0)

    def ready(t, p):
        for side in (0, 1):
            if t or side or p not in ends:
                x_copy(t, side, p).wait_recv()
            z_copy(t, side, p).wait_recv()
            if t >= 1:
                x_copy(t - 1, side, p).wait_send()

    def finish(t, p):
        if t + 1 < STEPS:
            for side in (0, 1):
                x_copy(t + 1, side, p).start()
                z_copy(t + 1, side, p).start()
        else:
            for by in range(1, slabs):
                s_copy(by, p).start()

    def combined(own, others):
        total = own[0]
        for other in others:
            total = total + other[0]
        mean = total * (1.0 / slabs)
        away = own[0] - mean
        squares, between = own[1], away * away
        for other in others:
            away = other[0] - mean
            squares, between = squares + other[1], between + away * away
        variance = (squares + depth * between) * (1.0 / (depth * slabs))
        return mean, lax.rsqrt(variance + 0.0001)

    def settle(p):
        for by in range(1, slabs):
            s_copy(by, p).wait_recv()
        lines[p, 0], lines[p, 1] = combined(
            (stats[p, 0], stats[p, 1]),
            [(stats_in[i, p, 0], stats_in[i, p, 1]) for i in range(slabs - 1)])

    for p in (0, last):
        stats[p] = jnp.zeros_like(stats[p])
    for t in range(STEPS):
        for p in range(1, last):
            ready(t, p)
            compute(t, p, 0, width)
            finish(t, p)
        ready(t, 0)
        ready(t, last)
        for k in range(chunks):
            tailed = t + 1 == STEPS and k + 1 == chunks
            if tailed:
                finish(t, 0)
                finish(t, last)
                for p in range(1, last):
                    settle(p)
            for side in sides:
                p = side * last
                if t == 0 and k + 1 == chunks:

                    def arrive(less, passed, side=side):
                        y_copy(0, side, chunks - 1, less).wait_recv()
                        if passed:
                            w_copy(side).wait_recv()

                    on_last(arrive)
                else:
                    y_copy(t, side, k).wait_recv()
                if t == 1 and k + 1 == chunks:

                    def left(less, _, side=side):
                        y_copy(0, 1 - side, chunks - 1, less).wait_send()

                    on_last(left)
                elif t >= 1:
                    y_copy(t - 1, 1 - side, k).wait_send()
                compute(t, p, spans[k][0], spans[k][1], side if tailed else None)
                if t + 1 < STEPS:
                    y_copy(t + 1, 1 - side, k).start()
        if t == 0 and forward:

            @pl.when(second)
            def _():
                for side in (0, 1):
                    w_copy(side).wait_send()

        if t + 1 < STEPS:
            finish(t, 0)
            finish(t, last)

    for by in range(1, slabs):
        e_copy(by).start()
    settle(0)
    settle(last)
    for by in range(1, slabs):
        e_copy(by).wait_recv()
    for side, p in ((0, 0), (1, last)):
        mean, scale = combined(
            (tail[side, 0], tail[side, 1]),
            [(tail_in[i, side, 0], tail_in[i, side, 1]) for i in range(slabs - 1)])
        lines[p, 0, width - short:width] = mean
        lines[p, 1, width - short:width] = scale

    for side in (0, 1):
        for k in range(chunks):
            y_copy(STEPS - 1, side, k).wait_send()
        for p in range(planes):
            x_copy(STEPS - 1, side, p).wait_send()
            for t in range(STEPS):
                z_copy(t, side, p).wait_send()
    for p in range(planes):
        for by in range(1, slabs):
            s_copy(by, p).wait_send()
    for by in range(1, slabs):
        e_copy(by).wait_send()


def scale_kernel(
    part, block, line, anomaly, out, scaled, out_sem, anomaly_sem
):
    planes, width = block.shape[:2]
    pieces = [(p, first) for p in range(planes) for first in range(0, width, part)]

    def copy(source, target, sems, i):
        p, first = pieces[i]
        at = (p, pl.ds(first, part))
        return pltpu.make_async_copy(source.at[at], target.at[at], sems.at[i])

    for i in range(len(pieces)):
        copy(block, out, out_sem, i).start()
    for i, (p, first) in enumerate(pieces):

        def row(x, _):
            centred = block[p, x] - line[p, 0, pl.ds(x, 1)]
            scaled[p, x] = centred * line[p, 1, pl.ds(x, 1)]
            return 0

        lax.fori_loop(first, first + part, row, 0)
        copy(scaled, anomaly, anomaly_sem, i).start()
    for i in range(len(pieces)):
        copy(block, out, out_sem, i).wait()
        copy(scaled, anomaly, anomaly_sem, i).wait()


def spans_of(width):
    short = min(2, width)
    first, spans = 0, []
    for i in range(3):
        size = (width - short - first) // (3 - i)
        if size:
            spans.append((first, size))
        first += size
    return tuple(spans) + ((first, width - first),)


def per_device(sizes, field_values, mobility, source):
    planes, width, depth, levels = field_values.shape
    slabs = sizes[2]
    spans = spans_of(width)
    chunks, short = len(spans), spans[-1][1]
    f32 = jnp.float32
    dma = pltpu.SemaphoreType.DMA
    any_space = pl.BlockSpec(memory_space=pl.ANY)
    held = pl.BlockSpec(memory_space=pltpu.VMEM)
    line = (planes, 2, width, levels)
    whole = jax.ShapeDtypeStruct(field_values.shape, f32)
    end, lines = pl.pallas_call(
        functools.partial(steps_kernel, sizes, spans),
        out_shape=(pltpu.VMEM(field_values.shape, f32), pltpu.VMEM(line, f32)),
        in_specs=[any_space] * 3,
        out_specs=(held, held),
        scratch_shapes=[
            pltpu.VMEM((2, planes + 2, width + 2, depth, levels), f32),
            pltpu.VMEM(field_values.shape, f32),
            pltpu.VMEM(field_values.shape, f32),
            pltpu.VMEM((STEPS, 2, planes, width, levels), f32),
            pltpu.VMEM((STEPS, 2, planes, width, levels), f32),
            pltpu.VMEM(line, f32),
            pltpu.VMEM((slabs - 1,) + line, f32),
            pltpu.VMEM((2, 2, short, levels), f32),
            pltpu.VMEM((slabs - 1, 2, 2, short, levels), f32),
            dma((STEPS, 2, chunks)), dma((STEPS, 2, chunks)),
            dma((2,)), dma((2,)),
            dma((STEPS, 2, planes)), dma((STEPS, 2, planes)),
            dma((STEPS, 2, planes)), dma((STEPS, 2, planes)),
            dma((slabs - 1, planes)), dma((slabs - 1, planes)),
            dma((slabs - 1,)), dma((slabs - 1,)),
            dma((4, planes)),
        ],
        compiler_params=pltpu.CompilerParams(
            collective_id=0, has_side_effects=True, vmem_limit_bytes=46 * 1024 * 1024),
    )(field_values, mobility, source)

    part = max(width // 4, 1)
    pieces = planes * (width // part)
    return pl.pallas_call(
        functools.partial(scale_kernel, part),
        out_shape=(whole, whole),
        in_specs=[held, held],
        out_specs=(any_space, any_space),
        scratch_shapes=[
            pltpu.VMEM(field_values.shape, f32),
            dma((pieces,)), dma((pieces,)),
        ],
        compiler_params=pltpu.CompilerParams(vmem_limit_bytes=20 * 1024 * 1024),
    )(end, lines)


def solution(mesh):
    sizes = tuple(mesh.shape[axis] for axis in ("rows", "cols", "slabs"))
    spec = P("rows", "cols", "slabs", None)
    return jax.shard_map(
        functools.partial(per_device, sizes),
        mesh=mesh,
        in_specs=(spec, spec, spec),
        out_specs=(spec, spec),
        check_vma=False,
    )
```
